128 devices in a mesh: ocn: 8 (over z, core), lon: 16 (over y, x).
Axes of the slice: x: 4, y: 4, z: 4, core: 2. Of those that a mesh axis runs over, the one named last changes fastest.
Arguments:
- ocean_state: bfloat16 [4, 12288, 128], P(None, ('ocn', 'lon')), may hold values from -6 to 6
- ice_cover: bfloat16 [12288, 128], P(('ocn', 'lon')), may hold values from 0 to 1
- ice_temp: bfloat16 [12288, 128], P(('ocn', 'lon')), may hold values from -6 to 6
- sea_mask: int32 [12288, 128], P(('ocn', 'lon')), may hold values from 0 to 1
- remap_tiles: bfloat16 [128, 640, 128, 128], P(('ocn', 'lon')), may hold values from 0 to 0.015625
- source_tile: int32 [128, 128, 5], P(('ocn', 'lon')), may hold values from 0 to 95
- send_block: int32 [128, 128, 5], P(('ocn', 'lon')), may hold values from -1 to 49, as said below
- recv_block: int32 [128, 128, 5], P(('ocn', 'lon')), may hold values from -1 to 49, as said below
- atm_state: float32 [4, 6400, 128], P(None, ('ocn', 'lon')), may hold values from -6 to 6
Outputs:
- ocean_fluxes: float32 [6, 12288, 128], P(None, ('ocn', 'lon'))
- atm_fluxes: float32 [6, 6400, 128], P(None, ('ocn', 'lon'))
The draws below stay inside these ranges and needn't reach their ends.
Inputs may be any that keep to these rules, and one draw needn't show every extreme that they name: `send_block`: -1 marks an empty slot; every slot from a device to itself is filled. recv_block[e, s, c] equals send_block[s, e, c].
All inputs are finite; a program needn't handle non-finite values.
Results may differ from the reference program's by a relative error of at most 0.0019.
Values may be sent and summed in bfloat16 or wider, within the bound.
No kernel may reach another device: no remote copies, remote signals or barrier semaphores. Data moves between devices by JAX's collectives and lax.ppermute only.
A program may use at most 64 MiB of HBM per device.

```python
import math
import jax
import jax.numpy as jnp
from jax import lax

TILE = 128
OB_DEV = 96
AB_DEV = 50
CAP = 5
OBT = 12288
ATB = 6400
SLOTS = 640
N_OCN = 8
N_LON = 16
DEVICES = 128


def intersection_table(key):
    base = jax.random.fold_in(key, 31)
    first, second = jax.random.split(base)
    sender = jnp.arange(DEVICES, dtype=jnp.int32)[:, None, None]
    target = jnp.arange(DEVICES, dtype=jnp.int32)[None, :, None]
    rolled = jax.random.randint(first, (DEVICES, DEVICES, CAP), 0, 100)
    limit = jnp.where(target // N_LON == N_OCN - 1, 95, 35)
    filled = (rolled < limit) | (sender == target)
    blocks = jax.random.randint(second, (DEVICES, DEVICES, CAP), 0, AB_DEV)
    return jnp.where(filled, blocks, -1).astype(jnp.int32)


def source_table(key):
    base = jax.random.fold_in(key, 47)
    return jax.random.randint(base, (DEVICES, DEVICES, CAP), 0, OB_DEV).astype(jnp.int32)


def draw_send_block(key, part):
    return intersection_table(key)


def draw_recv_block(key, part):
    return intersection_table(key).transpose(1, 0, 2)


def draw_source_tile(key, part):
    return source_table(key)


def draw_sea_mask(key, part):
    base = jax.random.fold_in(key, 61)
    first, second, third = jax.random.split(base, 3)
    coastal = jax.random.randint(first, (OBT, 1), 0, 100) < 4
    sparse = jax.random.randint(second, (OBT, 1), 0, 11)
    limit = jnp.where(coastal, sparse, 3 * TILE // 4)
    cells = jax.random.randint(third, (OBT, TILE), 0, TILE)
    return (cells < limit).astype(jnp.int32)


def draw_remap_tiles(key, part):
    base = jax.random.fold_in(key, 67)
    first, second, third, fourth = jax.random.split(base, 4)
    sources = source_table(key)
    blocks = intersection_table(key)
    ocean_weak = jax.random.randint(first, (DEVICES, OB_DEV), 0, 100) < 5
    atm_weak = jax.random.randint(second, (DEVICES, AB_DEV), 0, 100) < 5
    sender = jnp.arange(DEVICES, dtype=jnp.int32)[:, None, None]
    target = jnp.arange(DEVICES, dtype=jnp.int32)[None, :, None]
    partial_slot = ocean_weak[sender, sources] | atm_weak[target, jnp.maximum(blocks, 0)] & (blocks >= 0)
    factor = jnp.exp(jax.random.uniform(third, (DEVICES, DEVICES, CAP), jnp.float32, math.log(0.004), math.log(0.04)))
    scale = jnp.where(partial_slot, factor, 1.0).reshape(DEVICES, SLOTS, 1, 1)
    values = jax.random.uniform(fourth, (DEVICES, SLOTS, TILE, TILE), jnp.float32, 0.0, 2.0 / TILE)
    return (values * scale).astype(jnp.bfloat16)


def steps_of(stream_key, shape, cuts, least, top_value):
    level = 1.0
    for dim, blocks in cuts:
        steps = jax.random.uniform(jax.random.fold_in(jax.random.fold_in(stream_key, 6), dim), (blocks,), jnp.float32, least / len(cuts), top_value / len(cuts))
        level = level * jnp.repeat(jnp.exp(steps), shape[dim] // blocks).reshape((-1,) + (1,) * (len(shape) - 1 - dim))
    return level


def bell_draw(key, extent, spread, most, cuts=(), kind=jnp.bfloat16):
    gain = steps_of(key, extent, cuts, -0.22, 0.18) if cuts else 1.0
    result = jax.random.normal(key, extent, jnp.float32) * spread * gain
    return jnp.minimum(jnp.maximum(result, -most), most).astype(kind)


def setup_inputs(seed: int = 0) -> dict:
    key_of = jax.random.split(jax.random.key(seed), 10)
    ocean_state = bell_draw(key_of[0], (4, OBT, TILE), 1.0, 6.0, ((1, 128),))
    ice_cover = jnp.clip(1.0 * jax.random.uniform(key_of[1], (OBT, TILE), jnp.float32) ** steps_of(key_of[1], (OBT, TILE), ((0, 128),), -0.2, 0.2), 0.0, 1.0).astype(jnp.bfloat16)
    ice_temp = bell_draw(key_of[2], (OBT, TILE), 1.0, 6.0, ((0, 128),))
    sea_mask = draw_sea_mask(jax.random.fold_in(key_of[9], 71), 0)
    remap_tiles = draw_remap_tiles(jax.random.fold_in(key_of[9], 71), 0)
    source_tile = draw_source_tile(jax.random.fold_in(key_of[9], 71), 0)
    send_block = draw_send_block(jax.random.fold_in(key_of[9], 71), 0)
    recv_block = draw_recv_block(jax.random.fold_in(key_of[9], 71), 0)
    atm_state = bell_draw(key_of[8], (4, ATB, TILE), 1.0, 6.0, ((1, 128),), jnp.float32)
    return {"ocean_state": ocean_state, "ice_cover": ice_cover, "ice_temp": ice_temp, "sea_mask": sea_mask, "remap_tiles": remap_tiles, "source_tile": source_tile, "send_block": send_block, "recv_block": recv_block, "atm_state": atm_state}


highest = lax.Precision.HIGHEST

def stack_fields(ocean_state, ice_cover, ice_temp, sea_mask):
    sea_frac = sea_mask.astype(jnp.bfloat16)
    fields = jnp.concatenate([ocean_state, ice_cover[None], ice_temp[None]], 0)
    return jnp.concatenate([fields * sea_frac[None], sea_frac[None]], 0)

def bulk_fluxes(gathered, atm_state):
    inverse = 1.0 / jnp.maximum(gathered[6], 0.1)
    surface_temp = gathered[0] * inverse
    current_u = gathered[1] * inverse
    current_v = gathered[2] * inverse
    salinity = gathered[3] * inverse
    ice_frac = gathered[4] * inverse
    ice_surface = gathered[5] * inverse
    slip_east = atm_state[0] - current_u
    slip_north = atm_state[1] - current_v
    wind_speed = jnp.sqrt(slip_east * slip_east + slip_north * slip_north + 0.25)
    open_water = 1.0 - ice_frac
    saturation = 0.5 * jnp.exp(0.2 * surface_temp) * (1.0 - 0.05 * salinity)
    evaporation = 0.3 * open_water * wind_speed * (saturation - atm_state[3])
    heat = 0.3 * wind_speed * (open_water * (surface_temp - atm_state[2]) + ice_frac * (ice_surface - atm_state[2])) + 2.5 * evaporation
    return jnp.stack([0.5 * open_water * wind_speed * slip_east, 0.5 * open_water * wind_speed * slip_north, 0.8 * ice_frac * wind_speed * slip_east, 0.8 * ice_frac * wind_speed * slip_north, heat, evaporation], 0)

def reference(ocean_state, ice_cover, ice_temp, sea_mask, remap_tiles, source_tile, send_block, recv_block, atm_state):
    devices = remap_tiles.shape[0]
    slots = remap_tiles.shape[1]
    stacked = stack_fields(ocean_state, ice_cover, ice_temp, sea_mask)
    per_device = stacked.reshape(7, devices, OB_DEV, TILE).transpose(1, 0, 2, 3)
    sources = source_tile.reshape(devices, slots)
    targets = send_block.reshape(devices, slots)

    def forward(item):
        fields, tiles, sources_one, targets_one = item
        picked = jnp.take(fields, sources_one, axis=1).astype(jnp.float32)
        contrib = jnp.einsum('fsi,sij->sfj', picked, tiles.astype(jnp.float32), precision=highest)
        filled = (targets_one >= 0).astype(jnp.float32)
        return (contrib * filled[:, None, None]).astype(jnp.bfloat16)
    contribs = lax.map(forward, (per_device, remap_tiles, sources, targets))
    arriving = contribs.reshape(devices, devices, CAP, 7, TILE).transpose(1, 0, 2, 3, 4).reshape(devices, slots, 7, TILE)
    atm_dev = atm_state.reshape(4, devices, AB_DEV, TILE).transpose(1, 0, 2, 3)
    incoming = recv_block.reshape(devices, slots)

    def atmosphere(item):
        received, blocks, state = item
        onehot = (blocks[None, :] == jnp.arange(AB_DEV, dtype=jnp.int32)[:, None]).astype(jnp.float32)
        gathered = jnp.einsum('bs,sfj->fbj', onehot, received.astype(jnp.float32), precision=highest)
        fluxes = bulk_fluxes(gathered, state)
        back = jnp.einsum('bs,fbj->sfj', onehot, fluxes, precision=highest).astype(jnp.bfloat16)
        return (fluxes, back)
    fluxes, backs = lax.map(atmosphere, (arriving, incoming, atm_dev))
    returning = backs.reshape(devices, devices, CAP, 6, TILE).transpose(1, 0, 2, 3, 4).reshape(devices, slots, 6, TILE)
    sea_dev = sea_mask.reshape(devices, OB_DEV, TILE)

    def ocean(item):
        received, tiles, sources_one, targets_one, sea_one = item
        filled = (targets_one >= 0).astype(jnp.float32)
        onehot = (sources_one[None, :] == jnp.arange(OB_DEV, dtype=jnp.int32)[:, None]).astype(jnp.float32) * filled[None, :]
        tiles_wide = tiles.astype(jnp.float32)
        terms = jnp.einsum('sfj,sij->sfi', received.astype(jnp.float32), tiles_wide, precision=highest)
        coverage = lax.optimization_barrier(jnp.sum(tiles_wide, axis=2))
        summed = jnp.einsum('bs,sfi->fbi', onehot, terms, precision=highest)
        cover = jnp.dot(onehot, coverage, precision=highest)
        return summed / jnp.maximum(cover, 0.1)[None] * sea_one.astype(jnp.float32)[None]
    ocean_dev = lax.map(ocean, (returning, remap_tiles, sources, targets, sea_dev))
    ocean_fluxes = ocean_dev.transpose(1, 0, 2, 3).reshape(6, devices * OB_DEV, TILE)
    atm_fluxes = fluxes.transpose(1, 0, 2, 3).reshape(6, devices * AB_DEV, TILE)
    return (ocean_fluxes, atm_fluxes)
```

```python
import jax
import jax.numpy as jnp
from jax import lax
from jax.experimental import pallas as pl
from jax.experimental.pallas import tpu as pltpu
from jax.sharding import PartitionSpec as P

AXES = ("ocn", "lon")
MB = 1024 * 1024

PEER_BIT = 10
TILE_BIT = 18
GROUP = 16
CHUNKS = 16
SUMS = 4


def code_parts(code):
    slot = code & ((1 << PEER_BIT) - 1)
    peer = (code >> PEER_BIT) & ((1 << (TILE_BIT - PEER_BIT)) - 1)
    return slot, peer, code >> TILE_BIT


def forward_kernel(
    state_hbm,
    cover_hbm,
    temp_hbm,
    mask_hbm,
    tiles_hbm,
    source_hbm,
    target_hbm,
    kept,
    wire,
    listed,
    state,
    cover,
    temp,
    mask,
    source,
    target,
    fields,
    rows,
    sems,
    tile_sems,
):
    capacity, _, peers = target.shape
    slots = kept.shape[0]
    ocean_tiles = mask.shape[0]
    per_chunk = slots // CHUNKS
    peers_chunk = peers // CHUNKS
    wire_rows = wire.shape[0]
    small = (
        (source_hbm, source),
        (target_hbm, target),
        (mask_hbm, mask),
        (state_hbm, state),
        (cover_hbm, cover),
        (temp_hbm, temp),
    )
    copies = [pltpu.make_async_copy(a, b, sems.at[i]) for i, (a, b) in enumerate(small)]
    for copy in copies:
        copy.start()

    def chunk_copy(k):
        part = pl.ds(k * per_chunk, per_chunk)
        return pltpu.make_async_copy(tiles_hbm.at[part], kept.at[part], tile_sems.at[k])

    for k in range(CHUNKS):
        chunk_copy(k).start()
    for copy in copies:
        copy.wait()

    sea = mask[...].astype(jnp.float32)
    for f in range(4):
        fields[pl.ds(f, ocean_tiles, stride=8), :] = state[f].astype(jnp.float32) * sea
    fields[pl.ds(4, ocean_tiles, stride=8), :] = cover[...].astype(jnp.float32) * sea
    fields[pl.ds(5, ocean_tiles, stride=8), :] = temp[...].astype(jnp.float32) * sea
    fields[pl.ds(6, ocean_tiles, stride=8), :] = sea
    fields[pl.ds(7, ocean_tiles, stride=8), :] = jnp.zeros_like(sea)
    fields[8 * ocean_tiles :, :] = jnp.zeros((8, sea.shape[1]), jnp.float32)

    def list_peer(p, count):
        for c in range(capacity):
            tile = source[c, 0, p]
            listed[count] = (p * (capacity + (1 << PEER_BIT)) + c) + (tile << TILE_BIT)
            count = count + (target[c, 0, p] >= 0).astype(jnp.int32)
        return count

    count = lax.fori_loop(0, peers, list_peer, jnp.int32(0), unroll=4)
    spare = (slots - 1) + ((wire_rows - 7 * (slots - 1)) << PEER_BIT) + (ocean_tiles << TILE_BIT)
    for k in range(GROUP):
        listed[count + k] = spare
    groups = (count + (GROUP - 1)) // GROUP
    listed[slots + GROUP] = groups

    def wait_chunk(k, carry):
        chunk_copy(k).wait()
        return carry

    def group(g, waited):
        parts = [code_parts(listed[g * GROUP + k]) for k in range(GROUP)]
        need = jnp.minimum(parts[-1][1] // peers_chunk + 1, CHUNKS)
        lax.fori_loop(waited, need, wait_chunk, 0)
        for k in range(0, GROUP, 2):
            (s0, p0, t0), (s1, p1, t1) = parts[k], parts[k + 1]
            left = jnp.concatenate(
                [
                    fields[pl.ds(pl.multiple_of(t0 * 8, 8), 8), :],
                    fields[pl.ds(pl.multiple_of(t1 * 8, 8), 8), :],
                ],
                0,
            ).astype(jnp.bfloat16)
            right = jnp.concatenate([kept[s0], kept[s1]], 1)
            out = jnp.dot(left, right, preferred_element_type=jnp.float32)
            rows[pl.ds(7 * s0 + p0, 7), :] = out[0:7, 0:128]
            rows[pl.ds(7 * s1 + p1, 7), :] = out[8:15, 128:256]
        return jnp.maximum(waited, need)

    waited = lax.fori_loop(0, groups, group, jnp.int32(0))
    lax.fori_loop(waited, CHUNKS, wait_chunk, 0)
    step = wire_rows // 18

    def round_rows(i, carry):
        part = pl.ds(pl.multiple_of(i * step, 16), step)
        wire[part, :] = rows[part, :].astype(jnp.bfloat16)
        return carry

    lax.fori_loop(0, 18, round_rows, 0)


def atmosphere_kernel(
    arrived, block_hbm, state, fluxes, wire, block, wide, sums, table, out_rows, sem
):
    capacity, _, peers = block.shape
    atm_tiles = state.shape[0]
    copy = pltpu.make_async_copy(block_hbm, block, sem)
    copy.start()
    in_rows = arrived.shape[0]
    step = in_rows // 18

    def widen(i, carry):
        part = pl.ds(pl.multiple_of(i * step, 16), step)
        wide[part, :] = arrived[part, :].astype(jnp.float32)
        return carry

    lax.fori_loop(0, 18, widen, 0)
    for c in range(capacity):
        sums[c] = jnp.zeros(sums.shape[1:], jnp.float32)
    copy.wait()

    def tile_of(p, c):
        b = block[c, 0, p]
        return pl.multiple_of(jnp.where(b < 0, atm_tiles, b) * 8, 8)

    def gather(p, carry):
        for c in range(capacity):
            part = pl.ds(tile_of(p, c), 8)
            sums[c, part, :] = sums[c, part, :] + wide[pl.ds(p * 36 + c * 7, 8), :]
        return carry

    lax.fori_loop(0, peers, gather, 0, unroll=4)
    gathered = []
    for f in range(7):
        part = pl.ds(f, atm_tiles, stride=8)
        total = sums[0, part, :]
        for c in range(1, capacity):
            total = total + sums[c, part, :]
        gathered.append(total)
    inverse = 1.0 / jnp.maximum(gathered[6], 0.1)
    surface_temp, current_u, current_v, salinity, ice_frac, ice_surface = [
        g * inverse for g in gathered[:6]
    ]
    wind_u, wind_v, air_temp, humidity = [state[:, k, :] for k in range(4)]
    slip_east = wind_u - current_u
    slip_north = wind_v - current_v
    speed = jnp.sqrt(slip_east * slip_east + slip_north * slip_north + 0.25)
    open_water = 1.0 - ice_frac
    saturation = 0.5 * jnp.exp(0.2 * surface_temp) * (1.0 - 0.05 * salinity)
    evaporation = 0.3 * open_water * speed * (saturation - humidity)
    heat = (
        0.3
        * speed
        * (open_water * (surface_temp - air_temp) + ice_frac * (ice_surface - air_temp))
        + 2.5 * evaporation
    )
    results = (
        0.5 * open_water * speed * slip_east,
        0.5 * open_water * speed * slip_north,
        0.8 * ice_frac * speed * slip_east,
        0.8 * ice_frac * speed * slip_north,
        heat,
        evaporation,
    )
    for f, value in enumerate(results):
        fluxes[f] = value
        table[pl.ds(f, atm_tiles, stride=8), :] = value
    table[8 * atm_tiles :, :] = jnp.zeros((8, value.shape[1]), jnp.float32)

    def send(p, carry):
        for c in range(capacity):
            out_rows[pl.ds(p * 30 + c * 6, 6), :] = table[pl.ds(tile_of(p, c), 6), :]
        return carry

    lax.fori_loop(0, peers, send, 0, unroll=4)
    back_step = wire.shape[0] // 16

    def round_rows(i, carry):
        part = pl.ds(pl.multiple_of(i * back_step, 16), back_step)
        wire[part, :] = out_rows[part, :].astype(jnp.bfloat16)
        return carry

    lax.fori_loop(0, 16, round_rows, 0)


def ocean_kernel(returned, kept, list_hbm, mask, out, listed, wide, sums, sem):
    slots = kept.shape[0]
    ocean_tiles = mask.shape[0]
    copy = pltpu.make_async_copy(list_hbm, listed, sem)
    copy.start()
    in_rows = returned.shape[0]
    step = in_rows // 16

    def widen(i, carry):
        part = pl.ds(pl.multiple_of(i * step, 16), step)
        wide[part, :] = returned[part, :].astype(jnp.float32)
        return carry

    lax.fori_loop(0, 16, widen, 0)
    wide[in_rows:, :] = jnp.zeros((8, wide.shape[1]), jnp.float32)
    for k in range(SUMS):
        sums[k] = jnp.zeros(sums.shape[1:], jnp.float32)
    copy.wait()
    row = lax.broadcasted_iota(jnp.int32, (8, 128), 0)

    def group(g, carry):
        parts = [code_parts(listed[g * GROUP + k]) for k in range(GROUP)]
        for k in range(0, GROUP, 2):
            left = []
            for slot, _, _ in parts[k : k + 2]:
                values = wide[pl.ds(6 * slot, 8), :]
                left.append(jnp.where(row < 6, values, jnp.where(row == 6, 1.0, 0.0)))
            left = jnp.concatenate(left, 0).astype(jnp.bfloat16)
            right = jnp.concatenate([kept[parts[k][0]], kept[parts[k + 1][0]]], 0)
            terms = lax.dot_general(
                left, right, (((1,), (1,)), ((), ())), preferred_element_type=jnp.float32
            )
            for j in range(2):
                tile = parts[k + j][2]
                part = pl.ds(pl.multiple_of(tile * 8, 8), 8)
                n = (k + j) % SUMS
                sums[n, part, :] = (
                    sums[n, part, :] + terms[8 * j : 8 * j + 8, 128 * j : 128 * j + 128]
                )
        return carry

    lax.fori_loop(0, listed[slots + GROUP], group, 0)

    def total(f):
        part = pl.ds(f, ocean_tiles, stride=8)
        value = sums[0, part, :]
        for k in range(1, SUMS):
            value = value + sums[k, part, :]
        return value

    scale = mask[...].astype(jnp.float32) / jnp.maximum(total(6), 0.1)
    for f in range(6):
        out[f] = total(f) * scale


def anywhere():
    return pl.BlockSpec(memory_space=pl.ANY)


def in_vmem():
    return pl.BlockSpec(memory_space=pltpu.VMEM)


def exchange(rows, peers):
    wire = rows.reshape(peers, rows.shape[0] // (2 * peers), 2, rows.shape[1])
    arrived = lax.all_to_all(wire, AXES, split_axis=0, concat_axis=0, tiled=True)
    return arrived.reshape(rows.shape)


def shards(
    ocean_state,
    ice_cover,
    ice_temp,
    sea_mask,
    remap_tiles,
    source_tile,
    send_block,
    recv_block,
    atm_state,
):
    peers, capacity = send_block.shape[1:]
    slots = peers * capacity
    ocean_tiles, width = sea_mask.shape
    atm_tiles = atm_state.shape[1]
    source = source_tile.transpose(2, 0, 1)
    target = send_block.transpose(2, 0, 1)
    block = recv_block.transpose(2, 0, 1)
    list_size = slots + GROUP + 16
    kept, wire, listed = pl.pallas_call(
        forward_kernel,
        in_specs=[anywhere()] * 7,
        out_specs=[in_vmem(), in_vmem(), pl.BlockSpec(memory_space=pltpu.SMEM)],
        out_shape=[
            pltpu.VMEM((slots, width, width), jnp.bfloat16),
            jax.ShapeDtypeStruct((36 * peers, width), jnp.bfloat16),
            jax.ShapeDtypeStruct((list_size,), jnp.int32),
        ],
        scratch_shapes=[
            pltpu.VMEM(ocean_state.shape, jnp.bfloat16),
            pltpu.VMEM(ice_cover.shape, jnp.bfloat16),
            pltpu.VMEM(ice_temp.shape, jnp.bfloat16),
            pltpu.VMEM(sea_mask.shape, jnp.int32),
            pltpu.SMEM(source.shape, jnp.int32),
            pltpu.SMEM(target.shape, jnp.int32),
            pltpu.VMEM((8 * (ocean_tiles + 1), width), jnp.float32),
            pltpu.VMEM((36 * peers + 8, width), jnp.float32),
            pltpu.SemaphoreType.DMA((6,)),
            pltpu.SemaphoreType.DMA((CHUNKS,)),
        ],
        compiler_params=pltpu.CompilerParams(vmem_limit_bytes=16 * MB),
        name="forward",
    )(ocean_state, ice_cover, ice_temp, sea_mask, remap_tiles[0], source, target)
    arrived = exchange(wire, peers)
    fluxes, wire_back = pl.pallas_call(
        atmosphere_kernel,
        in_specs=[in_vmem(), anywhere(), in_vmem()],
        out_specs=[in_vmem(), in_vmem()],
        out_shape=[
            jax.ShapeDtypeStruct((6, atm_tiles, width), jnp.float32),
            jax.ShapeDtypeStruct((30 * peers, width), jnp.bfloat16),
        ],
        scratch_shapes=[
            pltpu.SMEM(block.shape, jnp.int32),
            pltpu.VMEM((36 * peers + 8, width), jnp.float32),
            pltpu.VMEM((capacity, 8 * (atm_tiles + 1), width), jnp.float32),
            pltpu.VMEM((8 * (atm_tiles + 1), width), jnp.float32),
            pltpu.VMEM((30 * peers, width), jnp.float32),
            pltpu.SemaphoreType.DMA,
        ],
        compiler_params=pltpu.CompilerParams(vmem_limit_bytes=16 * MB),
        name="atmosphere",
    )(arrived, block, atm_state.transpose(1, 0, 2))
    returned = exchange(wire_back, peers)
    ocean_fluxes = pl.pallas_call(
        ocean_kernel,
        in_specs=[in_vmem(), in_vmem(), anywhere(), in_vmem()],
        out_specs=in_vmem(),
        out_shape=jax.ShapeDtypeStruct((6, ocean_tiles, width), jnp.float32),
        scratch_shapes=[
            pltpu.SMEM((list_size,), jnp.int32),
            pltpu.VMEM((30 * peers + 8, width), jnp.float32),
            pltpu.VMEM((SUMS, 8 * (ocean_tiles + 1), width), jnp.float32),
            pltpu.SemaphoreType.DMA,
        ],
        compiler_params=pltpu.CompilerParams(vmem_limit_bytes=16 * MB),
        name="ocean",
    )(returned, kept, listed, sea_mask)
    return (ocean_fluxes, fluxes)


def solution(mesh):
    in_specs = (
        P(None, AXES, None),
        P(AXES, None),
        P(AXES, None),
        P(AXES, None),
        P(AXES, None, None, None),
        P(AXES, None, None),
        P(AXES, None, None),
        P(AXES, None, None),
        P(None, AXES, None),
    )
    out_specs = (P(None, AXES, None), P(None, AXES, None))
    return jax.shard_map(shards, mesh=mesh, in_specs=in_specs, out_specs=out_specs, check_vma=False)
```

```python
import jax
import jax.numpy as jnp
from jax import lax
from jax.experimental import pallas as pl
from jax.experimental.pallas import tpu as pltpu
from jax.sharding import PartitionSpec as P

AXES = ("ocn", "lon")
MB = 1024 * 1024

TILE_BIT = 10
GROUP = 32
CHUNKS = 16
SUMS = 4


def code_parts(code):
    return code & ((1 << TILE_BIT) - 1), code >> TILE_BIT


def forward_kernel(
    state_hbm,
    cover_hbm,
    temp_hbm,
    mask_hbm,
    tiles_hbm,
    source_hbm,
    target_hbm,
    kept,
    wire,
    listed,
    state,
    cover,
    temp,
    mask,
    source,
    target,
    fields,
    rows,
    counts,
    sems,
    tile_sems,
):
    capacity, _, peers = target.shape
    slots = kept.shape[0]
    ocean_tiles = mask.shape[0]
    peers_chunk = peers // CHUNKS
    wire_rows = wire.shape[0]
    small = (
        (source_hbm, source),
        (target_hbm, target),
        (mask_hbm, mask),
        (state_hbm, state),
        (cover_hbm, cover),
        (temp_hbm, temp),
    )
    copies = [pltpu.make_async_copy(a, b, sems.at[i]) for i, (a, b) in enumerate(small)]
    for copy in copies[:2]:
        copy.start()
    for copy in copies[2:]:
        copy.start()
    for copy in copies[:2]:
        copy.wait()

    def issue_chunk(k, carry):
        count = jnp.int32(0)
        for i in range(peers_chunk):
            for c in range(capacity):
                p = k * peers_chunk + i
                slot = p * capacity + c
                wanted = target[c, 0, p] >= 0

                @pl.when(wanted)
                def _():
                    pltpu.make_async_copy(
                        tiles_hbm.at[slot], kept.at[slot], tile_sems.at[k]
                    ).start()

                count = count + wanted.astype(jnp.int32)
        counts[k] = count
        return carry

    lax.fori_loop(0, CHUNKS, issue_chunk, 0)
    for copy in copies[2:]:
        copy.wait()

    sea = mask[...].astype(jnp.float32)
    for f in range(4):
        fields[pl.ds(f, ocean_tiles, stride=8), :] = state[f].astype(jnp.float32) * sea
    fields[pl.ds(4, ocean_tiles, stride=8), :] = cover[...].astype(jnp.float32) * sea
    fields[pl.ds(5, ocean_tiles, stride=8), :] = temp[...].astype(jnp.float32) * sea
    fields[pl.ds(6, ocean_tiles, stride=8), :] = sea
    fields[pl.ds(7, ocean_tiles, stride=8), :] = jnp.zeros_like(sea)

    def chunk(k, count):
        arrived = counts[k]

        @pl.when(arrived > 0)
        def _():
            part = pl.ds(0, arrived)
            pltpu.make_async_copy(tiles_hbm.at[part], kept.at[part], tile_sems.at[k]).wait()

        pairs = [(i, c) for i in range(peers_chunk) for c in range(capacity)]
        for n in range(0, len(pairs), 2):
            left, right, starts = [], [], []
            for i, c in pairs[n : n + 2]:
                p = k * peers_chunk + i
                slot = p * capacity + c
                tile = source[c, 0, p]
                listed[count] = slot + (tile << TILE_BIT)
                count = count + 1 + lax.shift_right_arithmetic(target[c, 0, p], 31)
                left.append(fields[pl.ds(pl.multiple_of(tile * 8, 8), 8), :])
                right.append(kept[slot])
                starts.append(p * 36 + c * 7)
            out = jnp.dot(
                jnp.concatenate(left, 0).astype(jnp.bfloat16),
                jnp.concatenate(right, 1),
                preferred_element_type=jnp.float32,
            )
            rows[pl.ds(starts[0], 7), :] = out[0:7, 0:128]
            rows[pl.ds(starts[1], 7), :] = out[8:15, 128:256]
        return count

    count = lax.fori_loop(0, CHUNKS, chunk, jnp.int32(0))
    spare = (slots - 1) + (ocean_tiles << TILE_BIT)
    for k in range(GROUP):
        listed[count + k] = spare
    listed[slots + GROUP] = (count + (GROUP - 1)) // GROUP
    step = wire_rows // 18

    def round_rows(i, carry):
        part = pl.ds(pl.multiple_of(i * step, 16), step)
        wire[part, :] = rows[part, :].astype(jnp.bfloat16)
        return carry

    lax.fori_loop(0, 18, round_rows, 0)


def atmosphere_kernel(
    arrived, block_hbm, state, fluxes_hbm, wire, block, wide, fluxes, table, out_rows, sem, *sums
):
    capacity, _, peers = block.shape
    atm_tiles = state.shape[0]
    copy = pltpu.make_async_copy(block_hbm, block, sem)
    copy.start()
    in_rows = arrived.shape[0]
    step = in_rows // 18

    def widen(i, carry):
        part = pl.ds(pl.multiple_of(i * step, 16), step)
        wide[part, :] = arrived[part, :].astype(jnp.float32)
        return carry

    lax.fori_loop(0, 18, widen, 0)
    for total in sums:
        total[...] = jnp.zeros(total.shape, jnp.float32)
    copy.wait()

    def tile_of(p, c):
        b = block[c, 0, p]
        return pl.multiple_of(jnp.where(b < 0, atm_tiles, b) * 8, 8)

    def gather(p, carry):
        for c in range(capacity):
            part = pl.ds(tile_of(p, c), 8)
            sums[c][part, :] = sums[c][part, :] + wide[pl.ds(p * 36 + c * 7, 8), :]
        return carry

    lax.fori_loop(0, peers, gather, 0, unroll=4)
    gathered = []
    for f in range(7):
        part = pl.ds(f, atm_tiles, stride=8)
        total = sums[0][part, :]
        for c in range(1, capacity):
            total = total + sums[c][part, :]
        gathered.append(total)
    inverse = 1.0 / jnp.maximum(gathered[6], 0.1)
    surface_temp, current_u, current_v, salinity, ice_frac, ice_surface = [
        g * inverse for g in gathered[:6]
    ]
    wind_u, wind_v, air_temp, humidity = [state[:, k, :] for k in range(4)]
    slip_east = wind_u - current_u
    slip_north = wind_v - current_v
    speed = jnp.sqrt(slip_east * slip_east + slip_north * slip_north + 0.25)
    open_water = 1.0 - ice_frac
    saturation = 0.5 * jnp.exp(0.2 * surface_temp) * (1.0 - 0.05 * salinity)
    evaporation = 0.3 * open_water * speed * (saturation - humidity)
    heat = (
        0.3
        * speed
        * (open_water * (surface_temp - air_temp) + ice_frac * (ice_surface - air_temp))
        + 2.5 * evaporation
    )
    results = (
        0.5 * open_water * speed * slip_east,
        0.5 * open_water * speed * slip_north,
        0.8 * ice_frac * speed * slip_east,
        0.8 * ice_frac * speed * slip_north,
        heat,
        evaporation,
    )
    for f, value in enumerate(results):
        fluxes[f] = value
        table[pl.ds(f, atm_tiles, stride=8), :] = value
    flux_copy = pltpu.make_async_copy(fluxes, fluxes_hbm, sem)
    flux_copy.start()
    table[8 * atm_tiles :, :] = jnp.zeros((8, value.shape[1]), jnp.float32)

    def send(p, carry):
        for c in range(capacity):
            out_rows[pl.ds(p * 30 + c * 6, 6), :] = table[pl.ds(tile_of(p, c), 6), :]
        return carry

    lax.fori_loop(0, peers, send, 0, unroll=4)
    back_step = wire.shape[0] // 16

    def round_rows(i, carry):
        part = pl.ds(pl.multiple_of(i * back_step, 16), back_step)
        wire[part, :] = out_rows[part, :].astype(jnp.bfloat16)
        return carry

    lax.fori_loop(0, 16, round_rows, 0)
    flux_copy.wait()


def ocean_kernel(returned, kept, list_hbm, mask, out_hbm, listed, wide, out, sem, out_sems, *sums):
    slots = kept.shape[0]
    ocean_tiles = mask.shape[0]
    copy = pltpu.make_async_copy(list_hbm, listed, sem)
    copy.start()
    in_rows = returned.shape[0]
    step = in_rows // 16

    def widen(i, carry):
        part = pl.ds(pl.multiple_of(i * step, 16), step)
        wide[part, :] = returned[part, :].astype(jnp.float32)
        return carry

    lax.fori_loop(0, 16, widen, 0)
    wide[in_rows:, :] = jnp.zeros((8, wide.shape[1]), jnp.float32)
    for total in sums:
        total[...] = jnp.zeros(total.shape, jnp.float32)
    copy.wait()
    row = lax.broadcasted_iota(jnp.int32, (8, 128), 0)

    def group(g, carry):
        parts = [code_parts(listed[g * GROUP + k]) for k in range(GROUP)]
        for k in range(0, GROUP, 2):
            left = []
            for slot, _ in parts[k : k + 2]:
                values = wide[pl.ds(6 * slot, 8), :]
                left.append(jnp.where(row < 6, values, jnp.where(row == 6, 1.0, 0.0)))
            left = jnp.concatenate(left, 0).astype(jnp.bfloat16)
            right = jnp.concatenate([kept[parts[k][0]], kept[parts[k + 1][0]]], 0)
            terms = lax.dot_general(
                left, right, (((1,), (1,)), ((), ())), preferred_element_type=jnp.float32
            )
            for j in range(2):
                tile = parts[k + j][1]
                part = pl.ds(pl.multiple_of(tile * 8, 8), 8)
                total = sums[(k + j) % SUMS]
                total[part, :] = (
                    total[part, :] + terms[8 * j : 8 * j + 8, 128 * j : 128 * j + 128]
                )
        return carry

    lax.fori_loop(0, listed[slots + GROUP], group, 0)

    def total(f):
        part = pl.ds(f, ocean_tiles, stride=8)
        value = sums[0][part, :]
        for k in range(1, SUMS):
            value = value + sums[k][part, :]
        return value

    scale = mask[...].astype(jnp.float32) / jnp.maximum(total(6), 0.1)
    copies = []
    for f in range(6):
        out[f] = total(f) * scale
        copies.append(pltpu.make_async_copy(out.at[f], out_hbm.at[f], out_sems.at[f]))
        copies[-1].start()
    for copy in copies:
        copy.wait()


def anywhere():
    return pl.BlockSpec(memory_space=pltpu.HBM)


def in_hbm(x):
    return pltpu.with_memory_space_constraint(x, pltpu.HBM)


def in_vmem():
    return pl.BlockSpec(memory_space=pltpu.VMEM)


def exchange(rows, peers):
    wire = rows.reshape(peers, rows.shape[0] // (2 * peers), 2, rows.shape[1])
    arrived = lax.all_to_all(wire, AXES, split_axis=0, concat_axis=0, tiled=True)
    return arrived.reshape(rows.shape)


def shards(
    ocean_state,
    ice_cover,
    ice_temp,
    sea_mask,
    remap_tiles,
    source_tile,
    send_block,
    recv_block,
    atm_state,
):
    peers, capacity = send_block.shape[1:]
    slots = peers * capacity
    ocean_tiles, width = sea_mask.shape
    atm_tiles = atm_state.shape[1]
    source = source_tile.transpose(2, 0, 1)
    target = send_block.transpose(2, 0, 1)
    block = recv_block.transpose(2, 0, 1)
    list_size = slots + GROUP + 16
    operands = (ocean_state, ice_cover, ice_temp, sea_mask, remap_tiles[0], source, target)
    kept, wire, listed = pl.pallas_call(
        forward_kernel,
        in_specs=[anywhere()] * 7,
        out_specs=[in_vmem(), in_vmem(), pl.BlockSpec(memory_space=pltpu.SMEM)],
        out_shape=[
            pltpu.VMEM((slots, width, width), jnp.bfloat16),
            jax.ShapeDtypeStruct((36 * peers, width), jnp.bfloat16),
            jax.ShapeDtypeStruct((list_size,), jnp.int32),
        ],
        scratch_shapes=[
            pltpu.VMEM(ocean_state.shape, jnp.bfloat16),
            pltpu.VMEM(ice_cover.shape, jnp.bfloat16),
            pltpu.VMEM(ice_temp.shape, jnp.bfloat16),
            pltpu.VMEM(sea_mask.shape, jnp.int32),
            pltpu.SMEM(source.shape, jnp.int32),
            pltpu.SMEM(target.shape, jnp.int32),
            pltpu.VMEM((8 * ocean_tiles, width), jnp.float32),
            pltpu.VMEM((36 * peers, width), jnp.float32),
            pltpu.SMEM((CHUNKS,), jnp.int32),
            pltpu.SemaphoreType.DMA((6,)),
            pltpu.SemaphoreType.DMA((CHUNKS,)),
        ],
        compiler_params=pltpu.CompilerParams(vmem_limit_bytes=16 * MB),
        name="forward",
    )(*[in_hbm(x) for x in operands])
    arrived = exchange(wire, peers)
    fluxes, wire_back = pl.pallas_call(
        atmosphere_kernel,
        in_specs=[in_vmem(), pl.BlockSpec(memory_space=pl.ANY), in_vmem()],
        out_specs=[anywhere(), in_vmem()],
        out_shape=[
            jax.ShapeDtypeStruct((6, atm_tiles, width), jnp.float32),
            jax.ShapeDtypeStruct((30 * peers, width), jnp.bfloat16),
        ],
        scratch_shapes=[
            pltpu.SMEM(block.shape, jnp.int32),
            pltpu.VMEM((36 * peers + 8, width), jnp.float32),
            pltpu.VMEM((6, atm_tiles, width), jnp.float32),
            pltpu.VMEM((8 * (atm_tiles + 1), width), jnp.float32),
            pltpu.VMEM((30 * peers, width), jnp.float32),
            pltpu.SemaphoreType.DMA,
        ]
        + [pltpu.VMEM((8 * (atm_tiles + 1), width), jnp.float32)] * capacity,
        compiler_params=pltpu.CompilerParams(vmem_limit_bytes=16 * MB),
        name="atmosphere",
    )(arrived, block, atm_state.transpose(1, 0, 2))
    returned = exchange(wire_back, peers)
    ocean_fluxes = pl.pallas_call(
        ocean_kernel,
        in_specs=[in_vmem(), in_vmem(), pl.BlockSpec(memory_space=pl.ANY), in_vmem()],
        out_specs=anywhere(),
        out_shape=jax.ShapeDtypeStruct((6, ocean_tiles, width), jnp.float32),
        scratch_shapes=[
            pltpu.SMEM((list_size,), jnp.int32),
            pltpu.VMEM((30 * peers + 8, width), jnp.float32),
            pltpu.VMEM((6, ocean_tiles, width), jnp.float32),
            pltpu.SemaphoreType.DMA,
            pltpu.SemaphoreType.DMA((6,)),
        ]
        + [pltpu.VMEM((8 * (ocean_tiles + 1), width), jnp.float32)] * SUMS,
        compiler_params=pltpu.CompilerParams(vmem_limit_bytes=16 * MB),
        name="ocean",
    )(returned, kept, listed, sea_mask)
    return (ocean_fluxes, fluxes)


def solution(mesh):
    in_specs = (
        P(None, AXES, None),
        P(AXES, None),
        P(AXES, None),
        P(AXES, None),
        P(AXES, None, None, None),
        P(AXES, None, None),
        P(AXES, None, None),
        P(AXES, None, None),
        P(None, AXES, None),
    )
    out_specs = (P(None, AXES, None), P(None, AXES, None))
    return jax.shard_map(shards, mesh=mesh, in_specs=in_specs, out_specs=out_specs, check_vma=False)
```

```python
import functools

import jax
import jax.numpy as jnp
from jax import lax
from jax.experimental import pallas as pl
from jax.experimental.pallas import tpu as pltpu
from jax.sharding import PartitionSpec as P

AXES = ("ocn", "lon")
MB = 1024 * 1024

GROUP = 104
CHUNKS = 4
WHOLE = 1
SUMS = 4
PARTIAL = 10


def forward_kernel(
    atm_tiles,
    state_hbm,
    cover_hbm,
    temp_hbm,
    mask_hbm,
    tiles_hbm,
    source_hbm,
    target_hbm,
    block_hbm,
    kept,
    wire,
    listed,
    place,
    state,
    cover,
    temp,
    mask,
    source,
    target,
    block,
    fields,
    rows,
    counts,
    sems,
    tile_sems,
):
    capacity, _, peers = target.shape
    ocean_tiles = mask.shape[0]
    peers_chunk = peers // CHUNKS
    wire_rows = wire.shape[0]
    small = (
        (source_hbm, source),
        (target_hbm, target),
        (mask_hbm, mask),
        (state_hbm, state),
        (cover_hbm, cover),
        (temp_hbm, temp),
        (block_hbm, block),
    )
    copies = [pltpu.make_async_copy(a, b, sems.at[i]) for i, (a, b) in enumerate(small)]
    for copy in copies[:2]:
        copy.start()
    for copy in copies[2:]:
        copy.start()
    per_chunk = peers_chunk * capacity
    for k in range(WHOLE):
        part = pl.ds(k * per_chunk, per_chunk)
        pltpu.make_async_copy(tiles_hbm.at[part], kept.at[part], tile_sems.at[k]).start()
        counts[k] = per_chunk
    for copy in copies[:2]:
        copy.wait()

    pairs = [(i, c) for i in range(peers_chunk) for c in range(capacity)]

    def list_tile(k, i, c, count, fetch):
        p = k * peers_chunk + i
        slot = p * capacity + c
        block_of = target[c, 0, p]
        listed[count] = p + c * peers
        if fetch:

            @pl.when(block_of >= 0)
            def _():
                pltpu.make_async_copy(tiles_hbm.at[slot], kept.at[slot], tile_sems.at[k]).start()

        return count + 1 + lax.shift_right_arithmetic(block_of, 31)

    def issue(k, count):
        first = count
        for i, c in pairs:
            count = list_tile(k, i, c, count, True)
        counts[k] = count - first
        return count

    count = jnp.int32(0)
    for k in range(WHOLE):
        for i, c in pairs:
            count = list_tile(k, i, c, count, False)
    for k in range(WHOLE, CHUNKS):
        count = issue(k, count)
    listed[kept.shape[0]] = count
    for copy in copies[2:]:
        copy.wait()

    place[...] = jnp.where(block[...] < 0, atm_tiles, block[...]) * 8
    sea = mask[...].astype(jnp.float32)
    for f in range(4):
        fields[pl.ds(f, ocean_tiles, stride=8), :] = state[f].astype(jnp.float32) * sea
    fields[pl.ds(4, ocean_tiles, stride=8), :] = cover[...].astype(jnp.float32) * sea
    fields[pl.ds(5, ocean_tiles, stride=8), :] = temp[...].astype(jnp.float32) * sea
    fields[pl.ds(6, ocean_tiles, stride=8), :] = sea
    fields[pl.ds(7, ocean_tiles, stride=8), :] = jnp.zeros_like(sea)

    def wait_chunk(k, carry):
        arriving = counts[k]

        @pl.when(arriving > 0)
        def _():
            part = pl.ds(0, arriving)
            pltpu.make_async_copy(tiles_hbm.at[part], kept.at[part], tile_sems.at[k]).wait()

        return carry

    def group(g, waited):
        codes = [listed[jnp.minimum(g * GROUP + k, count - 1)] for k in range(GROUP)]
        need = (codes[-1] & (peers - 1)) // peers_chunk + 1
        lax.fori_loop(waited, need, wait_chunk, 0)
        for k in range(0, GROUP, 2):
            left, right, starts = [], [], []
            for code in codes[k : k + 2]:
                p, c = code & (peers - 1), code >> (peers.bit_length() - 1)
                slot = p * capacity + c
                tile = source[c, 0, p]
                left.append(fields[pl.ds(pl.multiple_of(tile * 8, 8), 8), :])
                right.append(kept[slot])
                starts.append(7 * slot + p)
            out = jnp.dot(
                jnp.concatenate(left, 0).astype(jnp.bfloat16),
                jnp.concatenate(right, 1),
                preferred_element_type=jnp.float32,
            )
            rows[pl.ds(starts[0], 7), :] = out[0:7, 0:128]
            rows[pl.ds(starts[1], 7), :] = out[8:15, 128:256]
        return jnp.maximum(waited, need)

    waited = lax.fori_loop(0, (count + (GROUP - 1)) // GROUP, group, jnp.int32(0))
    lax.fori_loop(waited, CHUNKS, wait_chunk, 0)
    step = wire_rows // 18

    def round_rows(i, carry):
        part = pl.ds(pl.multiple_of(i * step, 16), step)
        wire[part, :] = rows[part, :].astype(jnp.bfloat16)
        return carry

    lax.fori_loop(0, 18, round_rows, 0)


def atmosphere_kernel(
    arrived, place_hbm, state, fluxes_hbm, wire, place, wide, fluxes, table, out_rows, sem, *sums
):
    capacity, _, peers = place.shape
    atm_tiles = state.shape[0]
    copy = pltpu.make_async_copy(place_hbm, place, sem)
    copy.start()
    in_rows = arrived.shape[0]
    step = in_rows // 18

    def widen(i, carry):
        part = pl.ds(pl.multiple_of(i * step, 16), step)
        wide[part, :] = arrived[part, :].astype(jnp.float32)
        return carry

    lax.fori_loop(0, 18, widen, 0)
    for total in sums:
        total[...] = jnp.zeros(total.shape, jnp.float32)
    copy.wait()

    def tile_of(p, c):
        return pl.multiple_of(place[c, 0, p], 8)

    for p in range(peers):
        for c in range(capacity):
            total = sums[(p * capacity + c) % PARTIAL]
            part = pl.ds(tile_of(p, c), 8)
            total[part, :] = total[part, :] + wide[p * 36 + c * 7 : p * 36 + c * 7 + 8, :]
    gathered = []
    for f in range(7):
        part = pl.ds(f, atm_tiles, stride=8)
        total = sums[0][part, :]
        for partial in sums[1:]:
            total = total + partial[part, :]
        gathered.append(total)
    inverse = 1.0 / jnp.maximum(gathered[6], 0.1)
    surface_temp, current_u, current_v, salinity, ice_frac, ice_surface = [
        g * inverse for g in gathered[:6]
    ]
    wind_u, wind_v, air_temp, humidity = [state[:, k, :] for k in range(4)]
    slip_east = wind_u - current_u
    slip_north = wind_v - current_v
    speed = jnp.sqrt(slip_east * slip_east + slip_north * slip_north + 0.25)
    open_water = 1.0 - ice_frac
    saturation = 0.5 * jnp.exp(0.2 * surface_temp) * (1.0 - 0.05 * salinity)
    evaporation = 0.3 * open_water * speed * (saturation - humidity)
    heat = (
        0.3
        * speed
        * (open_water * (surface_temp - air_temp) + ice_frac * (ice_surface - air_temp))
        + 2.5 * evaporation
    )
    results = (
        0.5 * open_water * speed * slip_east,
        0.5 * open_water * speed * slip_north,
        0.8 * ice_frac * speed * slip_east,
        0.8 * ice_frac * speed * slip_north,
        heat,
        evaporation,
    )
    for f, value in enumerate(results):
        fluxes[f] = value
        table[pl.ds(f, atm_tiles, stride=8), :] = value
    flux_copy = pltpu.make_async_copy(fluxes, fluxes_hbm, sem)
    flux_copy.start()
    table[8 * atm_tiles :, :] = jnp.zeros((8, value.shape[1]), jnp.float32)

    for p in range(peers):
        for c in range(capacity):
            start = p * 30 + c * 6
            out_rows[start : start + 6, :] = table[pl.ds(tile_of(p, c), 6), :]
    back_step = wire.shape[0] // 16

    def round_rows(i, carry):
        part = pl.ds(pl.multiple_of(i * back_step, 16), back_step)
        wire[part, :] = out_rows[part, :].astype(jnp.bfloat16)
        return carry

    lax.fori_loop(0, 16, round_rows, 0)
    flux_copy.wait()


def ocean_kernel(
    returned,
    kept,
    list_hbm,
    source_hbm,
    mask,
    out_hbm,
    listed,
    source,
    wide,
    out,
    sems,
    out_sems,
    *sums,
):
    capacity, _, peers = source.shape
    ocean_tiles = mask.shape[0]
    copies = [
        pltpu.make_async_copy(list_hbm, listed, sems.at[0]),
        pltpu.make_async_copy(source_hbm, source, sems.at[1]),
    ]
    for copy in copies:
        copy.start()
    in_rows = returned.shape[0]
    step = in_rows // 16

    def widen(i, carry):
        part = pl.ds(pl.multiple_of(i * step, 16), step)
        wide[part, :] = returned[part, :].astype(jnp.float32)
        return carry

    lax.fori_loop(0, 16, widen, 0)
    wide[in_rows:, :] = jnp.zeros((8, wide.shape[1]), jnp.float32)
    for total in sums:
        total[...] = jnp.zeros(total.shape, jnp.float32)
    for copy in copies:
        copy.wait()
    row = lax.broadcasted_iota(jnp.int32, (8, 128), 0)
    filled = listed[kept.shape[0]]

    def group(g, carry):
        for k in range(0, GROUP, 2):
            left, right, parts = [], [], []
            for n in (g * GROUP + k, g * GROUP + k + 1):
                code = listed[jnp.minimum(n, filled - 1)]
                p, c = code & (peers - 1), code >> (peers.bit_length() - 1)
                slot = p * capacity + c
                tile = jnp.where(n < filled, source[c, 0, p], ocean_tiles)
                values = wide[pl.ds(6 * slot, 8), :]
                left.append(jnp.where(row < 6, values, jnp.where(row == 6, 1.0, 0.0)))
                right.append(kept[slot])
                parts.append(pl.ds(pl.multiple_of(tile * 8, 8), 8))
            terms = lax.dot_general(
                jnp.concatenate(left, 0).astype(jnp.bfloat16),
                jnp.concatenate(right, 0),
                (((1,), (1,)), ((), ())),
                preferred_element_type=jnp.float32,
            )
            for j, part in enumerate(parts):
                total = sums[(k + j) % SUMS]
                total[part, :] = (
                    total[part, :] + terms[8 * j : 8 * j + 8, 128 * j : 128 * j + 128]
                )
        return carry

    lax.fori_loop(0, (filled + (GROUP - 1)) // GROUP, group, 0)

    def total(f):
        part = pl.ds(f, ocean_tiles, stride=8)
        value = sums[0][part, :]
        for k in range(1, SUMS):
            value = value + sums[k][part, :]
        return value

    scale = mask[...].astype(jnp.float32) / jnp.maximum(total(6), 0.1)
    copies = []
    for f in range(6):
        out[f] = total(f) * scale
        copies.append(pltpu.make_async_copy(out.at[f], out_hbm.at[f], out_sems.at[f]))
        copies[-1].start()
    for copy in copies:
        copy.wait()


def anywhere():
    return pl.BlockSpec(memory_space=pltpu.HBM)


def in_hbm(x):
    return pltpu.with_memory_space_constraint(x, pltpu.HBM)


def in_vmem():
    return pl.BlockSpec(memory_space=pltpu.VMEM)


def exchange(rows, peers):
    wire = rows.reshape(peers, rows.shape[0] // (2 * peers), 2, rows.shape[1])
    arrived = lax.all_to_all(wire, AXES, split_axis=0, concat_axis=0, tiled=True)
    return arrived.reshape(rows.shape)


def shards(
    ocean_state,
    ice_cover,
    ice_temp,
    sea_mask,
    remap_tiles,
    source_tile,
    send_block,
    recv_block,
    atm_state,
):
    peers, capacity = send_block.shape[1:]
    slots = peers * capacity
    ocean_tiles, width = sea_mask.shape
    atm_tiles = atm_state.shape[1]
    source = source_tile.transpose(2, 0, 1)
    target = send_block.transpose(2, 0, 1)
    block = recv_block.transpose(2, 0, 1)
    operands = (
        ocean_state,
        ice_cover,
        ice_temp,
        sea_mask,
        remap_tiles[0],
        source,
        target,
        block,
    )
    kept, wire, listed, place = pl.pallas_call(
        functools.partial(forward_kernel, atm_tiles),
        in_specs=[anywhere()] * 8,
        out_specs=[in_vmem(), in_vmem(), pl.BlockSpec(memory_space=pltpu.SMEM), in_vmem()],
        out_shape=[
            pltpu.VMEM((slots, width, width), jnp.bfloat16),
            jax.ShapeDtypeStruct((36 * peers, width), jnp.bfloat16),
            jax.ShapeDtypeStruct((slots + 8,), jnp.int32),
            jax.ShapeDtypeStruct(block.shape, jnp.int32),
        ],
        scratch_shapes=[
            pltpu.VMEM(ocean_state.shape, jnp.bfloat16),
            pltpu.VMEM(ice_cover.shape, jnp.bfloat16),
            pltpu.VMEM(ice_temp.shape, jnp.bfloat16),
            pltpu.VMEM(sea_mask.shape, jnp.int32),
            pltpu.SMEM(source.shape, jnp.int32),
            pltpu.SMEM(target.shape, jnp.int32),
            pltpu.VMEM(block.shape, jnp.int32),
            pltpu.VMEM((8 * ocean_tiles, width), jnp.float32),
            pltpu.VMEM((36 * peers, width), jnp.float32),
            pltpu.SMEM((CHUNKS,), jnp.int32),
            pltpu.SemaphoreType.DMA((7,)),
            pltpu.SemaphoreType.DMA((CHUNKS,)),
        ],
        compiler_params=pltpu.CompilerParams(vmem_limit_bytes=16 * MB),
        name="forward",
    )(*[in_hbm(x) for x in operands])
    arrived = exchange(wire, peers)
    fluxes, wire_back = pl.pallas_call(
        atmosphere_kernel,
        in_specs=[in_vmem(), pl.BlockSpec(memory_space=pl.ANY), in_vmem()],
        out_specs=[anywhere(), in_vmem()],
        out_shape=[
            jax.ShapeDtypeStruct((6, atm_tiles, width), jnp.float32),
            jax.ShapeDtypeStruct((30 * peers, width), jnp.bfloat16),
        ],
        scratch_shapes=[
            pltpu.SMEM(block.shape, jnp.int32),
            pltpu.VMEM((36 * peers + 8, width), jnp.float32),
            pltpu.VMEM((6, atm_tiles, width), jnp.float32),
            pltpu.VMEM((8 * (atm_tiles + 1), width), jnp.float32),
            pltpu.VMEM((30 * peers, width), jnp.float32),
            pltpu.SemaphoreType.DMA,
        ]
        + [pltpu.VMEM((8 * (atm_tiles + 1), width), jnp.float32)] * PARTIAL,
        compiler_params=pltpu.CompilerParams(vmem_limit_bytes=16 * MB),
        name="atmosphere",
    )(arrived, place, atm_state.transpose(1, 0, 2))
    returned = exchange(wire_back, peers)
    ocean_fluxes = pl.pallas_call(
        ocean_kernel,
        in_specs=[in_vmem(), in_vmem(), pl.BlockSpec(memory_space=pl.ANY), anywhere(), in_vmem()],
        out_specs=anywhere(),
        out_shape=jax.ShapeDtypeStruct((6, ocean_tiles, width), jnp.float32),
        scratch_shapes=[
            pltpu.SMEM(listed.shape, jnp.int32),
            pltpu.SMEM(source.shape, jnp.int32),
            pltpu.VMEM((30 * peers + 8, width), jnp.float32),
            pltpu.VMEM((6, ocean_tiles, width), jnp.float32),
            pltpu.SemaphoreType.DMA((2,)),
            pltpu.SemaphoreType.DMA((6,)),
        ]
        + [pltpu.VMEM((8 * (ocean_tiles + 1), width), jnp.float32)] * SUMS,
        compiler_params=pltpu.CompilerParams(vmem_limit_bytes=16 * MB),
        name="ocean",
    )(returned, kept, listed, in_hbm(source), sea_mask)
    return (ocean_fluxes, fluxes)


def solution(mesh):
    in_specs = (
        P(None, AXES, None),
        P(AXES, None),
        P(AXES, None),
        P(AXES, None),
        P(AXES, None, None, None),
        P(AXES, None, None),
        P(AXES, None, None),
        P(AXES, None, None),
        P(None, AXES, None),
    )
    out_specs = (P(None, AXES, None), P(None, AXES, None))
    return jax.shard_map(shards, mesh=mesh, in_specs=in_specs, out_specs=out_specs, check_vma=False)
```

```python
import functools

import jax
import jax.numpy as jnp
from jax import lax
from jax.experimental import pallas as pl
from jax.experimental.pallas import tpu as pltpu
from jax.sharding import PartitionSpec as P

AXES = ("ocn", "lon")
MB = 1024 * 1024

GROUP = 104
CHUNKS = 8
WHOLE = 1
SUMS = 4
PARTIAL = 10


def forward_kernel(
    atm_tiles,
    state_hbm,
    cover_hbm,
    temp_hbm,
    mask_hbm,
    tiles_hbm,
    source_hbm,
    target_hbm,
    block_hbm,
    kept,
    wire,
    listed_out,
    place,
    state,
    cover,
    temp,
    mask,
    source,
    target,
    block,
    fields,
    rows,
    listed,
    counts,
    sems,
    tile_sems,
):
    capacity, _, peers = target.shape
    ocean_tiles = mask.shape[0]
    peers_chunk = peers // CHUNKS
    wire_rows = wire.shape[0]
    small = (
        (target_hbm, target),
        (mask_hbm, mask),
        (state_hbm, state),
        (cover_hbm, cover),
        (temp_hbm, temp),
        (block_hbm, block),
    )
    copies = [pltpu.make_async_copy(a, b, sems.at[i]) for i, (a, b) in enumerate(small)]
    copies += [
        pltpu.make_async_copy(
            source_hbm.at[c, 0], source.at[pl.ds(c * peers, peers)], sems.at[len(small) + c]
        )
        for c in range(capacity)
    ]
    for copy in copies:
        copy.start()
    per_chunk = peers_chunk * capacity
    for k in range(WHOLE):
        part = pl.ds(k * per_chunk, per_chunk)
        pltpu.make_async_copy(tiles_hbm.at[part], kept.at[part], tile_sems.at[k]).start()
        counts[k] = per_chunk
    copies[0].wait()

    pairs = [(i, c) for i in range(peers_chunk) for c in range(capacity)]

    for k in range(WHOLE, CHUNKS):
        for i, c in pairs:
            p = k * peers_chunk + i
            slot = p * capacity + c

            @pl.when(target[c, 0, p] >= 0)
            def _():
                pltpu.make_async_copy(tiles_hbm.at[slot], kept.at[slot], tile_sems.at[k]).start()

    gaps = jnp.int32(0)
    for k in range(CHUNKS):
        first = gaps
        for n, (i, c) in enumerate(pairs):
            p = k * peers_chunk + i
            listed[gaps + (k * per_chunk + n)] = p + c * peers
            gaps = gaps + lax.shift_right_arithmetic(target[c, 0, p], 31)
        if k >= WHOLE:
            counts[k] = per_chunk + gaps - first
    count = gaps + kept.shape[0]
    for n in range(GROUP):
        listed[count + n] = capacity * peers - 1
    listed[kept.shape[0] + GROUP] = count
    list_copy = pltpu.make_async_copy(listed, listed_out, sems.at[len(small) + capacity])
    list_copy.start()
    for copy in copies[1:]:
        copy.wait()

    place[...] = jnp.where(block[...] < 0, atm_tiles, block[...]) * 8
    sea = mask[...].astype(jnp.float32)
    for f in range(4):
        fields[pl.ds(f, ocean_tiles, stride=8), :] = state[f].astype(jnp.float32) * sea
    fields[pl.ds(4, ocean_tiles, stride=8), :] = cover[...].astype(jnp.float32) * sea
    fields[pl.ds(5, ocean_tiles, stride=8), :] = temp[...].astype(jnp.float32) * sea
    fields[pl.ds(6, ocean_tiles, stride=8), :] = sea
    fields[pl.ds(7, ocean_tiles, stride=8), :] = jnp.zeros_like(sea)

    def wait_chunk(k, carry):
        arriving = counts[k]

        @pl.when(arriving > 0)
        def _():
            part = pl.ds(0, arriving)
            pltpu.make_async_copy(tiles_hbm.at[part], kept.at[part], tile_sems.at[k]).wait()

        return carry

    def group(g, waited):
        codes = [listed[g * GROUP + k] for k in range(GROUP)]
        need = (codes[-1] & (peers - 1)) // peers_chunk + 1
        lax.fori_loop(waited, need, wait_chunk, 0)
        for k in range(0, GROUP, 2):
            left, right, starts = [], [], []
            for code in codes[k : k + 2]:
                p, c = code & (peers - 1), code >> (peers.bit_length() - 1)
                slot = p * capacity + c
                tile = source[code]
                left.append(fields[pl.ds(pl.multiple_of(tile * 8, 8), 8), :])
                right.append(kept[slot])
                starts.append(7 * slot + p)
            out = jnp.dot(
                jnp.concatenate(left, 0).astype(jnp.bfloat16),
                jnp.concatenate(right, 1),
                preferred_element_type=jnp.float32,
            )
            rows[pl.ds(starts[0], 7), :] = out[0:7, 0:128]
            rows[pl.ds(starts[1], 7), :] = out[8:15, 128:256]
        return jnp.maximum(waited, need)

    waited = lax.fori_loop(0, (count + (GROUP - 1)) // GROUP, group, jnp.int32(0))
    lax.fori_loop(waited, CHUNKS, wait_chunk, 0)
    step = wire_rows // 18

    def round_rows(i, carry):
        part = pl.ds(pl.multiple_of(i * step, 16), step)
        wire[part, :] = rows[part, :].astype(jnp.bfloat16)
        return carry

    lax.fori_loop(0, 18, round_rows, 0)
    list_copy.wait()


def atmosphere_kernel(
    arrived, place_hbm, state, fluxes_hbm, wire, place, wide, fluxes, table, out_rows, sem, *sums
):
    capacity, _, peers = place.shape
    atm_tiles = state.shape[0]
    copy = pltpu.make_async_copy(place_hbm, place, sem)
    copy.start()
    in_rows = arrived.shape[0]
    step = in_rows // 18

    def widen(i, carry):
        part = pl.ds(pl.multiple_of(i * step, 16), step)
        wide[part, :] = arrived[part, :].astype(jnp.float32)
        return carry

    lax.fori_loop(0, 18, widen, 0)
    for total in sums:
        total[...] = jnp.zeros(total.shape, jnp.float32)
    copy.wait()

    def tile_of(p, c):
        return pl.multiple_of(place[c, 0, p], 8)

    for p in range(peers):
        for c in range(capacity):
            total = sums[(p * capacity + c) % PARTIAL]
            part = pl.ds(tile_of(p, c), 8)
            total[part, :] = total[part, :] + wide[p * 36 + c * 7 : p * 36 + c * 7 + 8, :]
    gathered = []
    for f in range(7):
        part = pl.ds(f, atm_tiles, stride=8)
        total = sums[0][part, :]
        for partial in sums[1:]:
            total = total + partial[part, :]
        gathered.append(total)
    inverse = 1.0 / jnp.maximum(gathered[6], 0.1)
    surface_temp, current_u, current_v, salinity, ice_frac, ice_surface = [
        g * inverse for g in gathered[:6]
    ]
    wind_u, wind_v, air_temp, humidity = [state[:, k, :] for k in range(4)]
    slip_east = wind_u - current_u
    slip_north = wind_v - current_v
    speed = jnp.sqrt(slip_east * slip_east + slip_north * slip_north + 0.25)
    open_water = 1.0 - ice_frac
    saturation = 0.5 * jnp.exp(0.2 * surface_temp) * (1.0 - 0.05 * salinity)
    evaporation = 0.3 * open_water * speed * (saturation - humidity)
    heat = (
        0.3
        * speed
        * (open_water * (surface_temp - air_temp) + ice_frac * (ice_surface - air_temp))
        + 2.5 * evaporation
    )
    results = (
        0.5 * open_water * speed * slip_east,
        0.5 * open_water * speed * slip_north,
        0.8 * ice_frac * speed * slip_east,
        0.8 * ice_frac * speed * slip_north,
        heat,
        evaporation,
    )
    for f, value in enumerate(results):
        fluxes[f] = value
        table[pl.ds(f, atm_tiles, stride=8), :] = value
    flux_copy = pltpu.make_async_copy(fluxes, fluxes_hbm, sem)
    flux_copy.start()
    table[8 * atm_tiles :, :] = jnp.zeros((8, value.shape[1]), jnp.float32)

    for p in range(peers):
        for c in range(capacity):
            start = p * 30 + c * 6
            out_rows[start : start + 6, :] = table[pl.ds(tile_of(p, c), 6), :]
    back_step = wire.shape[0] // 16

    def round_rows(i, carry):
        part = pl.ds(pl.multiple_of(i * back_step, 16), back_step)
        wire[part, :] = out_rows[part, :].astype(jnp.bfloat16)
        return carry

    lax.fori_loop(0, 16, round_rows, 0)
    flux_copy.wait()


def ocean_kernel(
    returned,
    kept,
    list_hbm,
    source_any,
    mask,
    out_hbm,
    listed,
    source,
    wide,
    out,
    sems,
    out_sems,
    *sums,
):
    capacity, _, peers = source_any.shape
    ocean_tiles = mask.shape[0]
    copies = [pltpu.make_async_copy(list_hbm, listed, sems.at[capacity])]
    copies += [
        pltpu.make_async_copy(source_any.at[c, 0], source.at[pl.ds(c * peers, peers)], sems.at[c])
        for c in range(capacity)
    ]
    for copy in copies:
        copy.start()
    in_rows = returned.shape[0]
    step = in_rows // 16

    def widen(i, carry):
        part = pl.ds(pl.multiple_of(i * step, 16), step)
        wide[part, :] = returned[part, :].astype(jnp.float32)
        return carry

    lax.fori_loop(0, 16, widen, 0)
    wide[in_rows:, :] = jnp.zeros((8, wide.shape[1]), jnp.float32)
    for total in sums:
        total[...] = jnp.zeros(total.shape, jnp.float32)
    for copy in copies:
        copy.wait()
    row = lax.broadcasted_iota(jnp.int32, (8, 128), 0)
    filled = listed[kept.shape[0] + GROUP]

    def group(g, carry):
        for k in range(0, GROUP, 2):
            left, right, parts = [], [], []
            for n in (g * GROUP + k, g * GROUP + k + 1):
                code = listed[n]
                p, c = code & (peers - 1), code >> (peers.bit_length() - 1)
                slot = p * capacity + c
                tile = jnp.where(n < filled, source[code], ocean_tiles)
                values = wide[pl.ds(6 * slot, 8), :]
                left.append(jnp.where(row < 6, values, jnp.where(row == 6, 1.0, 0.0)))
                right.append(kept[slot])
                parts.append(pl.ds(pl.multiple_of(tile * 8, 8), 8))
            terms = lax.dot_general(
                jnp.concatenate(left, 0).astype(jnp.bfloat16),
                jnp.concatenate(right, 0),
                (((1,), (1,)), ((), ())),
                preferred_element_type=jnp.float32,
            )
            for j, part in enumerate(parts):
                total = sums[(k + j) % SUMS]
                total[part, :] = (
                    total[part, :] + terms[8 * j : 8 * j + 8, 128 * j : 128 * j + 128]
                )
        return carry

    lax.fori_loop(0, (filled + (GROUP - 1)) // GROUP, group, 0)

    def total(f):
        part = pl.ds(f, ocean_tiles, stride=8)
        value = sums[0][part, :]
        for k in range(1, SUMS):
            value = value + sums[k][part, :]
        return value

    scale = mask[...].astype(jnp.float32) / jnp.maximum(total(6), 0.1)
    copies = []
    for f in range(6):
        out[f] = total(f) * scale
        copies.append(pltpu.make_async_copy(out.at[f], out_hbm.at[f], out_sems.at[f]))
        copies[-1].start()
    for copy in copies:
        copy.wait()


def anywhere():
    return pl.BlockSpec(memory_space=pltpu.HBM)


def in_hbm(x):
    return pltpu.with_memory_space_constraint(x, pltpu.HBM)


def in_vmem():
    return pl.BlockSpec(memory_space=pltpu.VMEM)


def exchange(rows, peers):
    wire = rows.reshape(peers, rows.shape[0] // (2 * peers), 2, rows.shape[1])
    arrived = lax.all_to_all(wire, AXES, split_axis=0, concat_axis=0, tiled=True)
    return arrived.reshape(rows.shape)


def shards(
    ocean_state,
    ice_cover,
    ice_temp,
    sea_mask,
    remap_tiles,
    source_tile,
    send_block,
    recv_block,
    atm_state,
):
    peers, capacity = send_block.shape[1:]
    slots = peers * capacity
    ocean_tiles, width = sea_mask.shape
    atm_tiles = atm_state.shape[1]
    source = source_tile.transpose(2, 0, 1)
    target = send_block.transpose(2, 0, 1)
    block = recv_block.transpose(2, 0, 1)
    list_size = -(-(slots + GROUP + 1) // 128) * 128
    operands = (
        ocean_state,
        ice_cover,
        ice_temp,
        sea_mask,
        remap_tiles[0],
        source,
        target,
        block,
    )
    kept, wire, listed, place = pl.pallas_call(
        functools.partial(forward_kernel, atm_tiles),
        in_specs=[anywhere()] * 8,
        out_specs=[in_vmem(), in_vmem(), pl.BlockSpec(memory_space=pl.ANY), in_vmem()],
        out_shape=[
            pltpu.VMEM((slots, width, width), jnp.bfloat16),
            jax.ShapeDtypeStruct((36 * peers, width), jnp.bfloat16),
            jax.ShapeDtypeStruct((list_size,), jnp.int32),
            jax.ShapeDtypeStruct(block.shape, jnp.int32),
        ],
        scratch_shapes=[
            pltpu.VMEM(ocean_state.shape, jnp.bfloat16),
            pltpu.VMEM(ice_cover.shape, jnp.bfloat16),
            pltpu.VMEM(ice_temp.shape, jnp.bfloat16),
            pltpu.VMEM(sea_mask.shape, jnp.int32),
            pltpu.SMEM((slots,), jnp.int32),
            pltpu.SMEM(target.shape, jnp.int32),
            pltpu.VMEM(block.shape, jnp.int32),
            pltpu.VMEM((8 * ocean_tiles, width), jnp.float32),
            pltpu.VMEM((36 * peers, width), jnp.float32),
            pltpu.SMEM((list_size,), jnp.int32),
            pltpu.SMEM((CHUNKS,), jnp.int32),
            pltpu.SemaphoreType.DMA((7 + capacity,)),
            pltpu.SemaphoreType.DMA((CHUNKS,)),
        ],
        compiler_params=pltpu.CompilerParams(vmem_limit_bytes=16 * MB),
        name="forward",
    )(*[in_hbm(x) for x in operands])
    arrived = exchange(wire, peers)
    fluxes, wire_back = pl.pallas_call(
        atmosphere_kernel,
        in_specs=[in_vmem(), pl.BlockSpec(memory_space=pl.ANY), in_vmem()],
        out_specs=[anywhere(), in_vmem()],
        out_shape=[
            jax.ShapeDtypeStruct((6, atm_tiles, width), jnp.float32),
            jax.ShapeDtypeStruct((30 * peers, width), jnp.bfloat16),
        ],
        scratch_shapes=[
            pltpu.SMEM(block.shape, jnp.int32),
            pltpu.VMEM((36 * peers + 8, width), jnp.float32),
            pltpu.VMEM((6, atm_tiles, width), jnp.float32),
            pltpu.VMEM((8 * (atm_tiles + 1), width), jnp.float32),
            pltpu.VMEM((30 * peers, width), jnp.float32),
            pltpu.SemaphoreType.DMA,
        ]
        + [pltpu.VMEM((8 * (atm_tiles + 1), width), jnp.float32)] * PARTIAL,
        compiler_params=pltpu.CompilerParams(vmem_limit_bytes=16 * MB),
        name="atmosphere",
    )(arrived, place, atm_state.transpose(1, 0, 2))
    returned = exchange(wire_back, peers)
    ocean_fluxes = pl.pallas_call(
        ocean_kernel,
        in_specs=[in_vmem(), in_vmem()] + [pl.BlockSpec(memory_space=pl.ANY)] * 2 + [in_vmem()],
        out_specs=anywhere(),
        out_shape=jax.ShapeDtypeStruct((6, ocean_tiles, width), jnp.float32),
        scratch_shapes=[
            pltpu.SMEM(listed.shape, jnp.int32),
            pltpu.SMEM((slots,), jnp.int32),
            pltpu.VMEM((30 * peers + 8, width), jnp.float32),
            pltpu.VMEM((6, ocean_tiles, width), jnp.float32),
            pltpu.SemaphoreType.DMA((1 + capacity,)),
            pltpu.SemaphoreType.DMA((6,)),
        ]
        + [pltpu.VMEM((8 * (ocean_tiles + 1), width), jnp.float32)] * SUMS,
        compiler_params=pltpu.CompilerParams(vmem_limit_bytes=16 * MB),
        name="ocean",
    )(returned, kept, listed, source, sea_mask)
    return (ocean_fluxes, fluxes)


def solution(mesh):
    in_specs = (
        P(None, AXES, None),
        P(AXES, None),
        P(AXES, None),
        P(AXES, None),
        P(AXES, None, None, None),
        P(AXES, None, None),
        P(AXES, None, None),
        P(AXES, None, None),
        P(None, AXES, None),
    )
    out_specs = (P(None, AXES, None), P(None, AXES, None))
    return jax.shard_map(shards, mesh=mesh, in_specs=in_specs, out_specs=out_specs, check_vma=False)
```

```python
import functools

import jax
import jax.numpy as jnp
from jax import lax
from jax.experimental import pallas as pl
from jax.experimental.pallas import tpu as pltpu
from jax.sharding import PartitionSpec as P

AXES = ("ocn", "lon")
MB = 1024 * 1024

GROUP = 104
CHUNKS = 8
WHOLE = 1
SUMS = 2
PARTIAL = 10


def forward_kernel(
    atm_tiles,
    state_hbm,
    cover_hbm,
    temp_hbm,
    mask_hbm,
    tiles_hbm,
    source_hbm,
    target_hbm,
    block_hbm,
    kept,
    wire,
    listed_out,
    place,
    state,
    cover,
    temp,
    mask,
    source,
    target,
    block,
    fields,
    rows,
    listed,
    counts,
    sems,
    tile_sems,
):
    capacity, _, peers = target.shape
    ocean_tiles = mask.shape[0]
    peers_chunk = peers // CHUNKS
    wire_rows = wire.shape[0]
    small = (
        (target_hbm, target),
        (mask_hbm, mask),
        (state_hbm, state),
        (cover_hbm, cover),
        (temp_hbm, temp),
        (block_hbm, block),
    )
    copies = [pltpu.make_async_copy(a, b, sems.at[i]) for i, (a, b) in enumerate(small)]
    copies += [
        pltpu.make_async_copy(
            source_hbm.at[c, 0], source.at[pl.ds(c * peers, peers)], sems.at[len(small) + c]
        )
        for c in range(capacity)
    ]
    for copy in copies:
        copy.start()
    per_chunk = peers_chunk * capacity
    for k in range(WHOLE):
        part = pl.ds(k * per_chunk, per_chunk)
        pltpu.make_async_copy(tiles_hbm.at[part], kept.at[part], tile_sems.at[k]).start()
        counts[k] = per_chunk
    copies[0].wait()

    pairs = [(i, c) for i in range(peers_chunk) for c in range(capacity)]

    for k in range(WHOLE, CHUNKS):
        for i, c in pairs:
            p = k * peers_chunk + i
            slot = p * capacity + c

            @pl.when(target[c, 0, p] >= 0)
            def _():
                pltpu.make_async_copy(tiles_hbm.at[slot], kept.at[slot], tile_sems.at[k]).start()

    for copy in copies[1:]:
        copy.wait()

    place[...] = jnp.where(block[...] < 0, atm_tiles, block[...]) * 8
    sea = mask[...].astype(jnp.float32)
    for f in range(4):
        fields[pl.ds(f, ocean_tiles, stride=8), :] = state[f].astype(jnp.float32) * sea
    fields[pl.ds(4, ocean_tiles, stride=8), :] = cover[...].astype(jnp.float32) * sea
    fields[pl.ds(5, ocean_tiles, stride=8), :] = temp[...].astype(jnp.float32) * sea
    fields[pl.ds(6, ocean_tiles, stride=8), :] = sea
    fields[pl.ds(7, ocean_tiles, stride=8), :] = jnp.zeros_like(sea)

    gaps = jnp.int32(0)
    for k in range(CHUNKS):
        first = gaps
        for n, (i, c) in enumerate(pairs):
            p = k * peers_chunk + i
            listed[gaps + (k * per_chunk + n)] = p + c * peers
            gaps = gaps + lax.shift_right_arithmetic(target[c, 0, p], 31)
        if k >= WHOLE:
            counts[k] = per_chunk + gaps - first
    count = gaps + kept.shape[0]
    for n in range(GROUP):
        listed[count + n] = capacity * peers - 1
    listed[kept.shape[0] + GROUP] = count
    list_copy = pltpu.make_async_copy(listed, listed_out, sems.at[len(small) + capacity])
    list_copy.start()

    def wait_chunk(k, carry):
        arriving = counts[k]

        @pl.when(arriving > 0)
        def _():
            part = pl.ds(0, arriving)
            pltpu.make_async_copy(tiles_hbm.at[part], kept.at[part], tile_sems.at[k]).wait()

        return carry

    def group(g, waited):
        codes = [listed[g * GROUP + k] for k in range(GROUP)]
        need = (codes[-1] & (peers - 1)) // peers_chunk + 1
        lax.fori_loop(waited, need, wait_chunk, 0)
        for k in range(0, GROUP, 2):
            left, right, starts = [], [], []
            for code in codes[k : k + 2]:
                p, c = code & (peers - 1), code >> (peers.bit_length() - 1)
                slot = p * capacity + c
                tile = source[code]
                left.append(fields[pl.ds(pl.multiple_of(tile * 8, 8), 8), :])
                right.append(kept[slot])
                starts.append(7 * slot + p)
            out = jnp.dot(
                jnp.concatenate(left, 0).astype(jnp.bfloat16),
                jnp.concatenate(right, 1),
                preferred_element_type=jnp.float32,
            )
            rows[pl.ds(starts[0], 7), :] = out[0:7, 0:128]
            rows[pl.ds(starts[1], 7), :] = out[8:15, 128:256]
        return jnp.maximum(waited, need)

    waited = lax.fori_loop(0, (count + (GROUP - 1)) // GROUP, group, jnp.int32(0))
    lax.fori_loop(waited, CHUNKS, wait_chunk, 0)
    step = wire_rows // 18

    def round_rows(i, carry):
        part = pl.ds(pl.multiple_of(i * step, 16), step)
        wire[part, :] = rows[part, :].astype(jnp.bfloat16)
        return carry

    lax.fori_loop(0, 18, round_rows, 0)
    list_copy.wait()


def atmosphere_kernel(
    arrived, place_hbm, state, fluxes_hbm, wire, place, wide, fluxes, table, out_rows, sem, *sums
):
    capacity, _, peers = place.shape
    atm_tiles = state.shape[0]
    copy = pltpu.make_async_copy(place_hbm, place, sem)
    copy.start()
    in_rows = arrived.shape[0]
    step = in_rows // 18

    def widen(i, carry):
        part = pl.ds(pl.multiple_of(i * step, 16), step)
        wide[part, :] = arrived[part, :].astype(jnp.float32)
        return carry

    lax.fori_loop(0, 18, widen, 0)
    for total in sums:
        total[...] = jnp.zeros(total.shape, jnp.float32)
    copy.wait()

    def tile_of(p, c):
        return pl.multiple_of(place[c, 0, p], 8)

    for p in range(peers):
        for c in range(capacity):
            total = sums[(p * capacity + c) % PARTIAL]
            part = pl.ds(tile_of(p, c), 8)
            total[part, :] = total[part, :] + wide[p * 36 + c * 7 : p * 36 + c * 7 + 8, :]
    together = sums[0][...]
    for partial in sums[1:]:
        together = together + partial[...]
    table[...] = together
    gathered = [table[pl.ds(f, atm_tiles, stride=8), :] for f in range(7)]
    inverse = 1.0 / jnp.maximum(gathered[6], 0.1)
    surface_temp, current_u, current_v, salinity, ice_frac, ice_surface = [
        g * inverse for g in gathered[:6]
    ]
    wind_u, wind_v, air_temp, humidity = [state[:, k, :] for k in range(4)]
    slip_east = wind_u - current_u
    slip_north = wind_v - current_v
    speed = jnp.sqrt(slip_east * slip_east + slip_north * slip_north + 0.25)
    open_water = 1.0 - ice_frac
    saturation = 0.5 * jnp.exp(0.2 * surface_temp) * (1.0 - 0.05 * salinity)
    evaporation = 0.3 * open_water * speed * (saturation - humidity)
    heat = (
        0.3
        * speed
        * (open_water * (surface_temp - air_temp) + ice_frac * (ice_surface - air_temp))
        + 2.5 * evaporation
    )
    results = (
        0.5 * open_water * speed * slip_east,
        0.5 * open_water * speed * slip_north,
        0.8 * ice_frac * speed * slip_east,
        0.8 * ice_frac * speed * slip_north,
        heat,
        evaporation,
    )
    for f, value in enumerate(results):
        fluxes[f] = value
        table[pl.ds(f, atm_tiles, stride=8), :] = value
    flux_copy = pltpu.make_async_copy(fluxes, fluxes_hbm, sem)
    flux_copy.start()
    table[8 * atm_tiles :, :] = jnp.zeros((8, value.shape[1]), jnp.float32)

    for p in range(peers):
        for c in range(capacity):
            start = p * 30 + c * 6
            out_rows[start : start + 6, :] = table[pl.ds(tile_of(p, c), 6), :]
    back_step = wire.shape[0] // 16

    def round_rows(i, carry):
        part = pl.ds(pl.multiple_of(i * back_step, 16), back_step)
        wire[part, :] = out_rows[part, :].astype(jnp.bfloat16)
        return carry

    lax.fori_loop(0, 16, round_rows, 0)
    flux_copy.wait()


def ocean_kernel(
    returned,
    kept,
    list_hbm,
    source_any,
    mask,
    out_hbm,
    listed,
    source,
    wide,
    out,
    sems,
    out_sems,
    *sums,
):
    capacity, _, peers = source_any.shape
    ocean_tiles = mask.shape[0]
    copies = [pltpu.make_async_copy(list_hbm, listed, sems.at[capacity])]
    copies += [
        pltpu.make_async_copy(source_any.at[c, 0], source.at[pl.ds(c * peers, peers)], sems.at[c])
        for c in range(capacity)
    ]
    for copy in copies:
        copy.start()
    in_rows = returned.shape[0]
    step = in_rows // 16

    def widen(i, carry):
        part = pl.ds(pl.multiple_of(i * step, 16), step)
        wide[part, :] = returned[part, :].astype(jnp.float32)
        return carry

    lax.fori_loop(0, 16, widen, 0)
    wide[in_rows:, :] = jnp.zeros((8, wide.shape[1]), jnp.float32)
    for total in sums:
        total[...] = jnp.zeros(total.shape, jnp.float32)
    for copy in copies:
        copy.wait()
    row = lax.broadcasted_iota(jnp.int32, (8, 128), 0)
    filled = listed[kept.shape[0] + GROUP]

    def group(g, carry):
        for k in range(0, GROUP, 2):
            left, right, parts = [], [], []
            for n in (g * GROUP + k, g * GROUP + k + 1):
                code = listed[n]
                p, c = code & (peers - 1), code >> (peers.bit_length() - 1)
                slot = p * capacity + c
                tile = jnp.where(n < filled, source[code], ocean_tiles)
                values = wide[pl.ds(6 * slot, 8), :]
                left.append(jnp.where(row < 6, values, jnp.where(row == 6, 1.0, 0.0)))
                right.append(kept[slot])
                parts.append(pl.ds(pl.multiple_of(tile * 8, 8), 8))
            terms = lax.dot_general(
                jnp.concatenate(left, 0).astype(jnp.bfloat16),
                jnp.concatenate(right, 0),
                (((1,), (1,)), ((), ())),
                preferred_element_type=jnp.float32,
            )
            for j, part in enumerate(parts):
                total = sums[(k + j) % SUMS]
                total[part, :] = (
                    total[part, :] + terms[8 * j : 8 * j + 8, 128 * j : 128 * j + 128]
                )
        return carry

    lax.fori_loop(0, (filled + (GROUP - 1)) // GROUP, group, 0)

    def total(f):
        part = pl.ds(f, ocean_tiles, stride=8)
        value = sums[0][part, :]
        for k in range(1, SUMS):
            value = value + sums[k][part, :]
        return value

    scale = mask[...].astype(jnp.float32) / jnp.maximum(total(6), 0.1)
    copies = []
    for f in range(6):
        out[f] = total(f) * scale
        copies.append(pltpu.make_async_copy(out.at[f], out_hbm.at[f], out_sems.at[f]))
        copies[-1].start()
    for copy in copies:
        copy.wait()


def anywhere():
    return pl.BlockSpec(memory_space=pltpu.HBM)


def in_hbm(x):
    return pltpu.with_memory_space_constraint(x, pltpu.HBM)


def in_vmem():
    return pl.BlockSpec(memory_space=pltpu.VMEM)


def exchange(rows, peers):
    wire = rows.reshape(peers, rows.shape[0] // (2 * peers), 2, rows.shape[1])
    arrived = lax.all_to_all(wire, AXES, split_axis=0, concat_axis=0, tiled=True)
    return arrived.reshape(rows.shape)


def shards(
    ocean_state,
    ice_cover,
    ice_temp,
    sea_mask,
    remap_tiles,
    source_tile,
    send_block,
    recv_block,
    atm_state,
):
    peers, capacity = send_block.shape[1:]
    slots = peers * capacity
    ocean_tiles, width = sea_mask.shape
    atm_tiles = atm_state.shape[1]
    source = source_tile.transpose(2, 0, 1)
    target = send_block.transpose(2, 0, 1)
    block = recv_block.transpose(2, 0, 1)
    list_size = -(-(slots + GROUP + 1) // 128) * 128
    operands = (
        ocean_state,
        ice_cover,
        ice_temp,
        sea_mask,
        remap_tiles[0],
        source,
        target,
        block,
    )
    kept, wire, listed, place = pl.pallas_call(
        functools.partial(forward_kernel, atm_tiles),
        in_specs=[anywhere()] * 8,
        out_specs=[in_vmem(), in_vmem(), pl.BlockSpec(memory_space=pl.ANY), in_vmem()],
        out_shape=[
            pltpu.VMEM((slots, width, width), jnp.bfloat16),
            jax.ShapeDtypeStruct((36 * peers, width), jnp.bfloat16),
            jax.ShapeDtypeStruct((list_size,), jnp.int32),
            jax.ShapeDtypeStruct(block.shape, jnp.int32),
        ],
        scratch_shapes=[
            pltpu.VMEM(ocean_state.shape, jnp.bfloat16),
            pltpu.VMEM(ice_cover.shape, jnp.bfloat16),
            pltpu.VMEM(ice_temp.shape, jnp.bfloat16),
            pltpu.VMEM(sea_mask.shape, jnp.int32),
            pltpu.SMEM((slots,), jnp.int32),
            pltpu.SMEM(target.shape, jnp.int32),
            pltpu.VMEM(block.shape, jnp.int32),
            pltpu.VMEM((8 * ocean_tiles, width), jnp.float32),
            pltpu.VMEM((36 * peers, width), jnp.float32),
            pltpu.SMEM((list_size,), jnp.int32),
            pltpu.SMEM((CHUNKS,), jnp.int32),
            pltpu.SemaphoreType.DMA((7 + capacity,)),
            pltpu.SemaphoreType.DMA((CHUNKS,)),
        ],
        compiler_params=pltpu.CompilerParams(vmem_limit_bytes=16 * MB),
        name="forward",
    )(*[in_hbm(x) for x in operands])
    arrived = exchange(wire, peers)
    fluxes, wire_back = pl.pallas_call(
        atmosphere_kernel,
        in_specs=[in_vmem(), pl.BlockSpec(memory_space=pl.ANY), in_vmem()],
        out_specs=[anywhere(), in_vmem()],
        out_shape=[
            jax.ShapeDtypeStruct((6, atm_tiles, width), jnp.float32),
            jax.ShapeDtypeStruct((30 * peers, width), jnp.bfloat16),
        ],
        scratch_shapes=[
            pltpu.SMEM(block.shape, jnp.int32),
            pltpu.VMEM((36 * peers + 8, width), jnp.float32),
            pltpu.VMEM((6, atm_tiles, width), jnp.float32),
            pltpu.VMEM((8 * (atm_tiles + 1), width), jnp.float32),
            pltpu.VMEM((30 * peers, width), jnp.float32),
            pltpu.SemaphoreType.DMA,
        ]
        + [pltpu.VMEM((8 * (atm_tiles + 1), width), jnp.float32)] * PARTIAL,
        compiler_params=pltpu.CompilerParams(vmem_limit_bytes=16 * MB),
        name="atmosphere",
    )(arrived, place, atm_state.transpose(1, 0, 2))
    returned = exchange(wire_back, peers)
    ocean_fluxes = pl.pallas_call(
        ocean_kernel,
        in_specs=[in_vmem(), in_vmem()] + [pl.BlockSpec(memory_space=pl.ANY)] * 2 + [in_vmem()],
        out_specs=anywhere(),
        out_shape=jax.ShapeDtypeStruct((6, ocean_tiles, width), jnp.float32),
        scratch_shapes=[
            pltpu.SMEM(listed.shape, jnp.int32),
            pltpu.SMEM((slots,), jnp.int32),
            pltpu.VMEM((30 * peers + 8, width), jnp.float32),
            pltpu.VMEM((6, ocean_tiles, width), jnp.float32),
            pltpu.SemaphoreType.DMA((1 + capacity,)),
            pltpu.SemaphoreType.DMA((6,)),
        ]
        + [pltpu.VMEM((8 * (ocean_tiles + 1), width), jnp.float32)] * SUMS,
        compiler_params=pltpu.CompilerParams(vmem_limit_bytes=16 * MB),
        name="ocean",
    )(returned, kept, listed, source, sea_mask)
    return (ocean_fluxes, fluxes)


def solution(mesh):
    in_specs = (
        P(None, AXES, None),
        P(AXES, None),
        P(AXES, None),
        P(AXES, None),
        P(AXES, None, None, None),
        P(AXES, None, None),
        P(AXES, None, None),
        P(AXES, None, None),
        P(None, AXES, None),
    )
    out_specs = (P(None, AXES, None), P(None, AXES, None))
    return jax.shard_map(shards, mesh=mesh, in_specs=in_specs, out_specs=out_specs, check_vma=False)
```
